8 devices in a mesh: replica: 1 (over z), pool: 8 (over y, x, core).
Axes of the slice: x: 2, y: 2, z: 1, core: 2. Of those that a mesh axis runs over, the one named last changes fastest.
Arguments:
- kv_pool: bfloat16 [2, 512, 2, 64, 8, 128], P(None, ('replica', 'pool'))
- page_idx: int32 [8, 8, 32], P(('replica', 'pool'))
- hidden: bfloat16 [8, 5120], P(('replica', 'pool'))
- norm_attn: bfloat16 [2, 5120], replicated
- norm_mlp: bfloat16 [2, 5120], replicated
- w_qkv: bfloat16 [2, 5120, 7168], replicated
- w_out: bfloat16 [2, 5120, 5120], replicated
- w_gate_up: bfloat16 [2, 5120, 27648], replicated
- w_down: bfloat16 [2, 13824, 5120], replicated
Outputs:
- output: bfloat16 [8, 5120], P(('replica', 'pool'))
All inputs are finite; a program needn't handle non-finite values.
Results may differ from the reference program's by a relative error of at most 0.0179669.
Values are sent between devices in bfloat16 or wider.
A program may use at most 4.25 GiB of HBM per device.

```python
import jax
import jax.numpy as jnp
from jax import lax

LAYERS = 2
GROUP_SIZE = 8
POOL_PAGES = 64
TAKE_PAGES = 32
PAGE_LEN = 64
WIDTH = 5120
FFN_WIDTH = 13824
HEADS = 40
KV_HEADS = 8
HEAD_DIM = 128

PREFIX_LEN = GROUP_SIZE * TAKE_PAGES * PAGE_LEN
Q_WIDTH = HEADS * HEAD_DIM
KV_WIDTH = KV_HEADS * HEAD_DIM
QKV_WIDTH = Q_WIDTH + 2 * KV_WIDTH
REPEAT = HEADS // KV_HEADS
NORM_EPS = 1e-5
ROPE_BASE = 500000.0


def setup_inputs(seed: int = 0, part: int = 0) -> dict:
    part_keys = jax.random.split(jax.random.fold_in(jax.random.key(seed), part), 4)
    shared_keys = jax.random.split(jax.random.key(seed + 1), 6)
    page_shape = (LAYERS, GROUP_SIZE * POOL_PAGES, 1, PAGE_LEN, KV_HEADS, HEAD_DIM)
    key_pages = jax.random.normal(part_keys[0], page_shape, jnp.float32)
    value_pages = jax.random.normal(part_keys[1], page_shape, jnp.float32) * (0.6 * PREFIX_LEN ** 0.5)
    kv_pool = jnp.concatenate([key_pages, value_pages], axis=2).astype(jnp.bfloat16)
    pair_keys = jax.random.split(part_keys[2], GROUP_SIZE * GROUP_SIZE)
    page_perm = jax.vmap(lambda pair_key: jax.random.permutation(pair_key, POOL_PAGES))(pair_keys)
    page_idx = page_perm[:, :TAKE_PAGES].reshape(GROUP_SIZE, GROUP_SIZE, TAKE_PAGES).astype(jnp.int32)
    hidden = jax.random.normal(part_keys[3], (GROUP_SIZE, WIDTH), jnp.float32).astype(jnp.bfloat16)
    norm_attn = jax.random.uniform(shared_keys[0], (LAYERS, WIDTH), jnp.float32, 0.5, 1.5).astype(jnp.bfloat16)
    norm_mlp = jax.random.uniform(shared_keys[1], (LAYERS, WIDTH), jnp.float32, 0.5, 1.5).astype(jnp.bfloat16)
    w_qkv = (jax.random.normal(shared_keys[2], (LAYERS, WIDTH, QKV_WIDTH), jnp.float32) * WIDTH ** -0.5).astype(jnp.bfloat16)
    w_out = (jax.random.normal(shared_keys[3], (LAYERS, Q_WIDTH, WIDTH), jnp.float32) * Q_WIDTH ** -0.5).astype(jnp.bfloat16)
    w_gate_up = (jax.random.normal(shared_keys[4], (LAYERS, WIDTH, 2 * FFN_WIDTH), jnp.float32) * WIDTH ** -0.5).astype(jnp.bfloat16)
    w_down = (jax.random.normal(shared_keys[5], (LAYERS, FFN_WIDTH, WIDTH), jnp.float32) * FFN_WIDTH ** -0.5).astype(jnp.bfloat16)
    return {'kv_pool': kv_pool, 'page_idx': page_idx, 'hidden': hidden, 'norm_attn': norm_attn, 'norm_mlp': norm_mlp, 'w_qkv': w_qkv, 'w_out': w_out, 'w_gate_up': w_gate_up, 'w_down': w_down}


def rms_norm(vec, gain):
    vec32 = vec.astype(jnp.float32)
    inv_rms = lax.rsqrt(jnp.mean(vec32 * vec32, axis=-1, keepdims=True) + NORM_EPS)
    return (vec32 * inv_rms * gain.astype(jnp.float32)).astype(jnp.bfloat16)


def rotary(heads_vec, position):
    half_dim = HEAD_DIM // 2
    inv_freq = ROPE_BASE ** (-jnp.arange(half_dim, dtype=jnp.float32) * 2.0 / HEAD_DIM)
    angle = position * inv_freq
    cos_part = jnp.cos(angle)
    sin_part = jnp.sin(angle)
    vec32 = heads_vec.astype(jnp.float32)
    first = vec32[..., :half_dim]
    second = vec32[..., half_dim:]
    return jnp.concatenate([first * cos_part - second * sin_part, second * cos_part + first * sin_part], axis=-1).astype(jnp.bfloat16)


def attend_one(queries, key_new, val_new, keys_pre, vals_pre):
    query32 = queries.astype(jnp.float32)
    score_scale = HEAD_DIM ** -0.5
    scores_pre = jnp.einsum('grd,ngd->grn', query32, keys_pre.astype(jnp.float32)) * score_scale
    scores_new = jnp.einsum('grd,gd->gr', query32, key_new.astype(jnp.float32)) * score_scale
    score_max = jnp.maximum(jnp.max(scores_pre, axis=-1), scores_new)
    exp_pre = jnp.exp(scores_pre - score_max[..., None])
    exp_new = jnp.exp(scores_new - score_max)
    denominator = jnp.sum(exp_pre, axis=-1) + exp_new
    prob_pre = (exp_pre / denominator[..., None]).astype(jnp.bfloat16)
    prob_new = (exp_new / denominator).astype(jnp.bfloat16)
    mixed = jnp.einsum('grn,ngd->grd', prob_pre.astype(jnp.float32), vals_pre.astype(jnp.float32))
    mixed = mixed + prob_new.astype(jnp.float32)[..., None] * val_new.astype(jnp.float32)[:, None, :]
    return mixed.astype(jnp.bfloat16)


def decode_layer(hidden, layer_inputs, page_idx):
    layer_pool, gain_attn, gain_mlp, w_qkv, w_out, w_gate_up, w_down = layer_inputs
    position = float(PREFIX_LEN)
    qkv_rows = jnp.dot(rms_norm(hidden, gain_attn), w_qkv, preferred_element_type=jnp.float32).astype(jnp.bfloat16)
    queries = rotary(qkv_rows[:, :Q_WIDTH].reshape(GROUP_SIZE, KV_HEADS, REPEAT, HEAD_DIM), position)
    key_new = rotary(qkv_rows[:, Q_WIDTH:Q_WIDTH + KV_WIDTH].reshape(GROUP_SIZE, KV_HEADS, HEAD_DIM), position)
    val_new = qkv_rows[:, Q_WIDTH + KV_WIDTH:].reshape(GROUP_SIZE, KV_HEADS, HEAD_DIM)
    owner_base = jnp.arange(GROUP_SIZE, dtype=jnp.int32)[:, None] * POOL_PAGES

    def one_request(request_inputs):
        query_one, key_one, val_one, idx_one = request_inputs
        pages = jnp.take(layer_pool, (idx_one + owner_base).reshape(-1), axis=0)
        keys_pre = pages[:, 0].reshape(PREFIX_LEN, KV_HEADS, HEAD_DIM)
        vals_pre = pages[:, 1].reshape(PREFIX_LEN, KV_HEADS, HEAD_DIM)
        return attend_one(query_one, key_one, val_one, keys_pre, vals_pre)

    attn_out = lax.map(one_request, (queries, key_new, val_new, page_idx)).reshape(GROUP_SIZE, Q_WIDTH)
    attn_proj = jnp.dot(attn_out, w_out, preferred_element_type=jnp.float32)
    hidden_mid = (hidden.astype(jnp.float32) + attn_proj).astype(jnp.bfloat16)
    gate_up = jnp.dot(rms_norm(hidden_mid, gain_mlp), w_gate_up, preferred_element_type=jnp.float32).astype(jnp.bfloat16)
    ffn_act = (jax.nn.silu(gate_up[:, :FFN_WIDTH].astype(jnp.float32)) * gate_up[:, FFN_WIDTH:].astype(jnp.float32)).astype(jnp.bfloat16)
    ffn_out = jnp.dot(ffn_act, w_down, preferred_element_type=jnp.float32)
    return (hidden_mid.astype(jnp.float32) + ffn_out).astype(jnp.bfloat16)


def reference(kv_pool, page_idx, hidden, norm_attn, norm_mlp, w_qkv, w_out, w_gate_up, w_down):
    def scan_body(carry, layer_inputs):
        return decode_layer(carry, layer_inputs, page_idx), None
    return lax.scan(scan_body, hidden, (kv_pool, norm_attn, norm_mlp, w_qkv, w_out, w_gate_up, w_down))[0]
```

```python
import functools
import math

import jax
import jax.numpy as jnp
import numpy as np
from jax import lax
from jax.experimental import pallas as pl
from jax.experimental.pallas import tpu as pltpu
from jax.sharding import PartitionSpec as P

NORM_EPS = 1e-5
ROPE_BASE = 500000.0
NEG = -3.0e38
MESH = pl.DeviceIdType.MESH
F32 = jnp.float32
BF16 = jnp.bfloat16

N_DEV = 8
GU_SLOTS = 3
DN_SLOTS = 4
STEP = 256
PAGES_PER_ITER = 16


def rope_table(position, head_dim):
    half = head_dim // 2
    freq = ROPE_BASE ** (-np.arange(half, dtype=np.float64) * 2.0 / head_dim)
    angle = position * freq
    cos = np.concatenate([np.cos(angle), np.cos(angle)])
    sin = np.concatenate([-np.sin(angle), np.sin(angle)])
    return np.stack([cos, sin]).astype(np.float32)


def kernel(dims, kv, pidx, hid, na, nm, rope, wqkv, wout, wgu, wdn, o,
           wq_b, k_b, v_b, wo_b, gu_b, dn_b, s_b,
           hid_v, na_v, nm_v, pidx_v, rope_v, x0, xf, xm, qbuf, psend, precv,
           abuf, mbuf, msend, mrecv, maskx, mrow, snew, vnew_b,
           sm_sem, wq_sem, k_sem, v_sem, wo_sem, gu_sem, dn_sem,
           x0_s, x0_r, mk_s, mk_r, q_s, q_r, p_s, p_r, a_s, a_r, xm_s, xm_r, xf_s, xf_r, m_s, m_r):
    layers, pages, page_len, kv_heads, head_dim, rep_q, width, ffn, steps = dims
    pairs = kv_heads // 2
    slice_w = width // N_DEV
    q_w = rep_q * head_dim
    rows = rep_q * N_DEV
    scale2 = float(head_dim ** -0.5 * math.log2(math.e))

    me = lax.axis_index('pool')
    rep = lax.axis_index('replica')
    b0 = lax.rem(me, 2)
    b1 = lax.rem(me // 2, 2)
    b2 = me // 4

    def peer(k):
        return lax.rem(b0 + k % 2, 2) + 2 * lax.rem(b1 + (k // 2) % 2, 2) + 4 * lax.rem(b2 + k // 4, 2)

    def pair_of(kx):
        return lax.rem(b1 + kx % 2, 2) + 2 * lax.rem(b2 + kx // 2, 2)

    def remote(src, dst, ssem, rsem, k):
        return pltpu.make_async_remote_copy(src_ref=src, dst_ref=dst, send_sem=ssem, recv_sem=rsem,
                                            device_id=(rep, peer(k)), device_id_type=MESH)

    FAR_FIRST = (6, 7, 4, 5, 2, 3, 1)

    def my_cols(ref, w):
        return ref.at[:, pl.ds(pl.multiple_of(me * w, 128), w)]

    def wq_copies(l):
        out = []
        base = 0
        for i, (off, w) in enumerate(((0, q_w), (width, head_dim), (width + kv_heads * head_dim, head_dim))):
            src = wqkv.at[l, :, pl.ds(pl.multiple_of(off + me * w, 128), w)]
            out.append(pltpu.make_async_copy(src, wq_b.at[:, pl.ds(base, w)], wq_sem.at[i]))
            base += w
        return out

    def kv_copies(l, which, buf, sem):
        return [pltpu.make_async_copy(kv.at[l, :, which, :, p], buf.at[p], sem.at[p]) for p in range(pairs)]

    def wo_copy(l):
        return pltpu.make_async_copy(wout.at[l, :, pl.ds(pl.multiple_of(me * slice_w, 128), slice_w)], wo_b, wo_sem.at[0])

    def ffn_base(dev):
        return 128 * ((dev * (ffn // 128)) // N_DEV)

    def gu_copies(l, s):
        slot = lax.rem(l * steps + s, GU_SLOTS)
        return [pltpu.make_async_copy(
            wgu.at[l, :, pl.ds(pl.multiple_of(part * ffn + ffn_base(me) + s * STEP, 128), STEP)],
            gu_b.at[slot, part], gu_sem.at[slot, part]) for part in range(2)]

    def dn_copies(l, s):
        slot = lax.rem(l * steps + s, DN_SLOTS)
        return [pltpu.make_async_copy(
            wdn.at[l, pl.ds(pl.multiple_of(ffn_base(j) + s * STEP, 128), STEP),
                   pl.ds(pl.multiple_of(me * slice_w, 128), slice_w)],
            dn_b.at[slot, pl.ds(j * STEP, STEP)], dn_sem.at[slot, j]) for j in range(N_DEV)]

    def start(cps):
        for c in cps:
            c.start()

    def wait(cps):
        for c in cps:
            c.wait()

    small = [pltpu.make_async_copy(a, b, sm_sem.at[i]) for i, (a, b) in enumerate(
        ((hid, hid_v), (pidx.at[0], pidx_v), (na, na_v), (nm, nm_v), (rope, rope_v)))]
    start(small)
    start(wq_copies(0))
    start(kv_copies(0, 0, k_b, k_sem))

    barrier = pltpu.get_barrier_semaphore()
    for k in range(1, N_DEV):
        pl.semaphore_signal(barrier, inc=1, device_id=(rep, peer(k)), device_id_type=MESH)
    wait(small)
    x0[me] = hid_v[...].astype(F32)
    lane = lax.broadcasted_iota(jnp.int32, (N_DEV, 128), 1)
    idx = pidx_v[...]
    hit = lane < 0
    for j in range(idx.shape[1]):
        hit = jnp.logical_or(hit, idx[:, j:j + 1] == lane)
    hitf = jnp.where(hit, 1.0, 0.0).astype(F32)
    for owner in range(N_DEV):
        msend[owner] = jnp.broadcast_to(hitf[owner:owner + 1, :], (N_DEV, 128))
    pl.semaphore_wait(barrier, N_DEV - 1)
    x0_cps = [remote(x0.at[me], x0.at[me], x0_s.at[k], x0_r.at[k], k) for k in FAR_FIRST]
    start(x0_cps)
    mk_cps = [remote(msend.at[peer(k)], mrecv.at[me], mk_s.at[k], mk_r.at[k], k) for k in FAR_FIRST]
    start(mk_cps)
    mrecv[me] = msend[me]
    start(kv_copies(0, 1, v_b, v_sem))
    wait(x0_cps)
    sub8 = lax.broadcasted_iota(jnp.int32, (N_DEV, width), 0)
    xin = jnp.zeros((N_DEV, width), F32)
    for j in range(N_DEV):
        xin = jnp.where(sub8 == j, jnp.broadcast_to(x0[j], (N_DEV, width)), xin)
    xf[...] = xin.astype(BF16)

    odd = lax.rem(lax.broadcasted_iota(jnp.int32, (rows, 128), 1), 2) == 1
    grp = lax.broadcasted_iota(jnp.int32, (N_DEV, 128), 1) // 16
    low8 = lax.rem(lax.broadcasted_iota(jnp.int32, (N_DEV, 128), 1), 16) < 8

    def norm(x, gains, l):
        g = jnp.where(l == 0, gains[0:1, :].astype(F32), gains[1:2, :].astype(F32))
        inv = lax.rsqrt(jnp.sum(x * x, axis=-1, keepdims=True) / width + NORM_EPS)
        return (x * inv * g).astype(BF16)

    def layer(l, carry):
        h = norm(xf[...].astype(F32), na_v[...], l)
        wait(wq_copies(l))
        u = jnp.dot(h, wq_b[...], preferred_element_type=F32).astype(BF16).astype(F32)

        @pl.when(l == 0)
        def _():
            start([wo_copy(0)])
            for s in range(GU_SLOTS):
                start(gu_copies(0, s))
            for s in range(DN_SLOTS):
                start(dn_copies(0, s))

        @pl.when(l + 1 < layers)
        def _():
            start(wq_copies(l + 1))

        cos = rope_v[0:1, :]
        sin = rope_v[1:2, :]

        def rot(v):
            return (v * cos + pltpu.roll(v, head_dim // 2, 1) * sin).astype(BF16)

        qs = [rot(u[:, g * head_dim:(g + 1) * head_dim]).astype(F32) for g in range(rep_q)]
        kn = rot(u[:, q_w:q_w + head_dim]).astype(F32)
        vnew_b[...] = u[:, q_w + head_dim:]
        qbuf[me] = jnp.concatenate(qs, axis=0).astype(BF16)
        q_cps = {k: remote(qbuf.at[me], qbuf.at[me], q_s.at[k], q_r.at[k], k) for k in range(1, N_DEV)}
        start([q_cps[k] for k in FAR_FIRST])
        for g in range(rep_q):
            snew[g] = jnp.broadcast_to(jnp.sum(qs[g] * kn, axis=-1, keepdims=True), (N_DEV, 128))

        @pl.when(l == 0)
        def _():
            wait(mk_cps)
            sub = lax.broadcasted_iota(jnp.int32, (N_DEV, 128), 0)
            mk = jnp.zeros((N_DEV, 128), F32)
            for r in range(N_DEV):
                mk = jnp.where(sub == r, mrecv[r], mk)
            for p in range(pages):
                maskx[p] = jnp.broadcast_to(mk[:, p:p + 1], (N_DEV, 128))

        wait(kv_copies(l, 0, k_b, k_sem))
        flat = PAGES_PER_ITER * page_len * 2
        for kx in range(pairs):
            for k in (2 * kx, 2 * kx + 1):
                if k:
                    q_cps[k].wait()
            p = pair_of(kx)
            q2 = jnp.concatenate([qbuf[2 * p], qbuf[2 * p + 1]], axis=0)

            def score_body(c, mx, p=p, q2=q2, kx=kx):
                kt = k_b[p, pl.ds(c * PAGES_PER_ITER, PAGES_PER_ITER)].reshape(flat, head_dim)
                s = lax.dot_general(q2, kt, (((1,), (1,)), ((), ())), preferred_element_type=F32)
                for i in range(PAGES_PER_ITER):
                    cols = slice(i * 128, (i + 1) * 128)
                    keep = maskx[c * PAGES_PER_ITER + i] > 0.5
                    keep = jnp.concatenate([keep] * rep_q, axis=0)
                    sp = jnp.where(odd, s[rows:, cols], s[:rows, cols])
                    sp = jnp.where(keep, sp, NEG)
                    s_b[kx, c * PAGES_PER_ITER + i] = sp
                    mx = jnp.maximum(mx, sp)
                return mx

            mx = lax.fori_loop(0, pages // PAGES_PER_ITER, score_body, jnp.full((rows, 128), NEG, F32))
            m_e = jnp.max(jnp.where(odd, NEG, mx), axis=-1, keepdims=True)
            m_o = jnp.max(jnp.where(odd, mx, NEG), axis=-1, keepdims=True)
            mrow[kx] = jnp.where(odd, m_o, m_e)

        @pl.when(l + 1 < layers)
        def _():
            start(kv_copies(l + 1, 0, k_b, k_sem))

        wait(kv_copies(l, 1, v_b, v_sem))
        p_cps = {k: remote(psend.at[peer(k)], precv.at[me], p_s.at[k], p_r.at[k], k) for k in range(1, N_DEV)}
        for kx in reversed(range(pairs)):
            p = pair_of(kx)
            m = mrow[kx]

            def value_body(c, carry, p=p, m=m, kx=kx):
                acc, den = carry
                pieces = []
                for i in range(PAGES_PER_ITER):
                    e = jnp.exp2((s_b[kx, c * PAGES_PER_ITER + i] - m) * scale2)
                    den = den + e
                    pieces.append(jnp.concatenate([jnp.where(odd, 0.0, e), jnp.where(odd, e, 0.0)], axis=0).astype(BF16))
                vt = v_b[p, pl.ds(c * PAGES_PER_ITER, PAGES_PER_ITER)].reshape(flat, head_dim)
                acc = acc + jnp.dot(jnp.concatenate(pieces, axis=1), vt, preferred_element_type=F32)
                return acc, den

            acc, den = lax.fori_loop(0, pages // PAGES_PER_ITER, value_body,
                                     (jnp.zeros((2 * rows, head_dim), F32), jnp.zeros((rows, 128), F32)))
            for hh in range(2):
                par = odd if hh else jnp.logical_not(odd)
                l_h = jnp.sum(jnp.where(par, den, 0.0), axis=-1, keepdims=True)
                m_h = jnp.max(jnp.where(par, m, NEG), axis=-1, keepdims=True)
                stat = jnp.zeros((N_DEV, 128), F32)
                for g in range(rep_q):
                    rs = slice(g * N_DEV, (g + 1) * N_DEV)
                    psend[2 * p + hh, g] = acc[hh * rows + g * N_DEV:hh * rows + (g + 1) * N_DEV]
                    stat = jnp.where(grp == g, jnp.where(low8, m_h[rs], l_h[rs]), stat)
                psend[2 * p + hh, rep_q] = stat
            for k in (2 * kx, 2 * kx + 1):
                if k:
                    p_cps[k].start()
        precv[me] = psend[me]

        @pl.when(l + 1 < layers)
        def _():
            start(kv_copies(l + 1, 1, v_b, v_sem))

        wait([p_cps[k] for k in FAR_FIRST])
        stats = [precv[j, rep_q] for j in range(N_DEV)]
        heads_out = []
        for g in range(rep_q):
            ms = [jnp.broadcast_to(st[:, 16 * g:16 * g + 1], (N_DEV, 128)) for st in stats]
            ls = [jnp.broadcast_to(st[:, 16 * g + 8:16 * g + 9], (N_DEV, 128)) for st in stats]
            sn = snew[g]
            top = sn
            for mj in ms:
                top = jnp.maximum(top, mj)
            e_new = jnp.exp2((sn - top) * scale2)
            den = e_new
            num = jnp.zeros((N_DEV, head_dim), F32)
            for j in range(N_DEV):
                w = jnp.exp2((ms[j] - top) * scale2)
                den = den + w * ls[j]
                num = num + w * precv[j, g]
            p_new = (e_new / den).astype(BF16).astype(F32)
            heads_out.append(num / den + p_new * vnew_b[...])
        my_cols(abuf, q_w)[...] = jnp.concatenate(heads_out, axis=1).astype(BF16)
        a_cps = [remote(my_cols(abuf, q_w), my_cols(abuf, q_w), a_s.at[k], a_r.at[k], k) for k in FAR_FIRST]
        start(a_cps)
        wait([wo_copy(l)])
        wait(a_cps)

        proj = jnp.dot(abuf[...], wo_b[...], preferred_element_type=F32)
        my_cols(xm, slice_w)[...] = (my_cols(xf, slice_w)[...].astype(F32) + proj).astype(BF16)
        xm_cps = [remote(my_cols(xm, slice_w), my_cols(xm, slice_w), xm_s.at[k], xm_r.at[k], k) for k in FAR_FIRST]
        start(xm_cps)
        wait(xm_cps)

        h2 = norm(xm[...].astype(F32), nm_v[...], l)
        mlane = lax.broadcasted_iota(jnp.int32, (N_DEV, STEP), 1)

        def m_cps(s):
            cols = pl.ds(pl.multiple_of(me * STEP, 128), STEP)
            return [remote(mbuf.at[s, :, cols], mbuf.at[s, :, cols], m_s.at[s, k], m_r.at[s, k], k) for k in FAR_FIRST]

        def up_body(s, carry):
            slot = lax.rem(l * steps + s, GU_SLOTS)
            wait(gu_copies(l, s))
            gate = jnp.dot(h2, gu_b[slot, 0], preferred_element_type=F32).astype(BF16).astype(F32)
            up = jnp.dot(h2, gu_b[slot, 1], preferred_element_type=F32).astype(BF16).astype(F32)
            act = gate / (1.0 + jnp.exp(-gate)) * up
            dup = jnp.logical_and(jnp.logical_and(b0 == 1, s == 0), mlane < 128)
            act = jnp.where(dup, 0.0, act).astype(BF16)
            mbuf[s, :, pl.ds(pl.multiple_of(me * STEP, 128), STEP)] = act
            start(m_cps(s))

            @pl.when(s + GU_SLOTS < steps)
            def _():
                start(gu_copies(l, s + GU_SLOTS))
            return carry

        lax.fori_loop(0, steps, up_body, 0)

        def down_body(s, acc):
            slot = lax.rem(l * steps + s, DN_SLOTS)
            wait(dn_copies(l, s))
            wait(m_cps(s))
            acc = acc + jnp.dot(mbuf[s], dn_b[slot], preferred_element_type=F32)

            @pl.when(s + DN_SLOTS < steps)
            def _():
                start(dn_copies(l, s + DN_SLOTS))
            return acc

        acc = lax.fori_loop(0, steps, down_body, jnp.zeros((N_DEV, slice_w), F32))
        my_cols(xf, slice_w)[...] = (my_cols(xm, slice_w)[...].astype(F32) + acc).astype(BF16)
        xf_cps = [remote(my_cols(xf, slice_w), my_cols(xf, slice_w), xf_s.at[k], xf_r.at[k], k) for k in FAR_FIRST]
        start(xf_cps)

        @pl.when(l + 1 < layers)
        def _():
            start([wo_copy(l + 1)])
            for s in range(GU_SLOTS):
                start(gu_copies(l + 1, s))
            for s in range(DN_SLOTS):
                start(dn_copies(l + 1, s))

        wait(xf_cps)
        return carry

    lax.fori_loop(0, layers, layer, 0)
    xo = xf[...].astype(F32)
    o[...] = jnp.sum(jnp.where(sub8 == me, xo, 0.0), axis=0, keepdims=True).astype(BF16)


def solution(mesh):
    def device_fn(kv_pool, page_idx, hidden, norm_attn, norm_mlp, w_qkv, w_out, w_gate_up, w_down):
        layers, pages, _, page_len, kv_heads, head_dim = kv_pool.shape
        group, take = page_idx.shape[1:]
        width = hidden.shape[1]
        ffn = w_down.shape[1]
        rep_q = (w_qkv.shape[2] - 2 * kv_heads * head_dim) // head_dim // kv_heads
        rows = rep_q * group
        slice_w = width // group
        q_w = rep_q * head_dim
        steps = -(-(-(-(ffn // 128) // group)) // (STEP // 128))
        position = float(group * take * page_len)
        rope = jnp.asarray(rope_table(position, head_dim))
        kv = kv_pool.reshape(layers, pages, 2, page_len, kv_heads // 2, 2, head_dim)
        dims = (layers, pages, page_len, kv_heads, head_dim, rep_q, width, ffn, steps)
        dma = pltpu.SemaphoreType.DMA
        any_spec = pl.BlockSpec(memory_space=pl.ANY)
        pairs = kv_heads // 2
        return pl.pallas_call(
            functools.partial(kernel, dims),
            out_shape=jax.ShapeDtypeStruct((1, width), BF16),
            in_specs=[any_spec] * 10,
            out_specs=pl.BlockSpec(memory_space=pltpu.VMEM),
            scratch_shapes=[
                pltpu.VMEM((width, q_w + 2 * head_dim), BF16),
                pltpu.VMEM((pairs, pages, page_len, 2, head_dim), BF16),
                pltpu.VMEM((pairs, pages, page_len, 2, head_dim), BF16),
                pltpu.VMEM((width, slice_w), BF16),
                pltpu.VMEM((GU_SLOTS, 2, width, STEP), BF16),
                pltpu.VMEM((DN_SLOTS, group * STEP, slice_w), BF16),
                pltpu.VMEM((pairs, pages, rows, 128), F32),
                pltpu.VMEM((1, width), BF16),
                pltpu.VMEM((layers, width), BF16),
                pltpu.VMEM((layers, width), BF16),
                pltpu.VMEM((group, take), jnp.int32),
                pltpu.VMEM((2, head_dim), F32),
                pltpu.VMEM((group, 1, width), F32),
                pltpu.VMEM((group, width), BF16),
                pltpu.VMEM((group, width), BF16),
                pltpu.VMEM((group, rows, head_dim), BF16),
                pltpu.VMEM((group, rep_q + 1, group, 128), F32),
                pltpu.VMEM((group, rep_q + 1, group, 128), F32),
                pltpu.VMEM((group, width), BF16),
                pltpu.VMEM((steps, group, group * STEP), BF16),
                pltpu.VMEM((group, group, 128), F32),
                pltpu.VMEM((group, group, 128), F32),
                pltpu.VMEM((pages, group, 128), F32),
                pltpu.VMEM((pairs, rows, 128), F32),
                pltpu.VMEM((rep_q, group, 128), F32),
                pltpu.VMEM((group, head_dim), F32),
                dma((5,)), dma((3,)), dma((pairs,)), dma((pairs,)), dma((1,)),
                dma((GU_SLOTS, 2)), dma((DN_SLOTS, group)),
            ] + [dma((group,))] * 14 + [dma((steps, group))] * 2,
            compiler_params=pltpu.CompilerParams(
                collective_id=0, has_side_effects=True, vmem_limit_bytes=67_043_328),
            name="decode_step",
        )(kv, page_idx, hidden, norm_attn, norm_mlp, rope, w_qkv, w_out, w_gate_up, w_down)

    row_spec = P(('replica', 'pool'))
    in_specs = (P(None, ('replica', 'pool')), row_spec, row_spec, P(), P(), P(), P(), P(), P())
    return jax.shard_map(device_fn, mesh=mesh, in_specs=in_specs, out_specs=row_spec, check_vma=False)
```

```python
import functools
import math

import jax
import jax.numpy as jnp
import numpy as np
from jax import lax
from jax.experimental import pallas as pl
from jax.experimental.pallas import tpu as pltpu
from jax.sharding import PartitionSpec as P

NORM_EPS = 1e-5
ROPE_BASE = 500000.0
NEG = -3.0e38
MESH = pl.DeviceIdType.MESH
F32 = jnp.float32
BF16 = jnp.bfloat16

N_DEV = 8
RING = 7
STEP = 256
HEADS_PER_GROUP = 4
SCORE_PAGES = 32
VALUE_PAGES = 32


def rope_table(position, head_dim):
    half = head_dim // 2
    freq = ROPE_BASE ** (-np.arange(half, dtype=np.float64) * 2.0 / head_dim)
    angle = position * freq
    cos = np.concatenate([np.cos(angle), np.cos(angle)])
    sin = np.concatenate([-np.sin(angle), np.sin(angle)])
    return np.stack([cos, sin]).astype(np.float32)


def kernel(dims, kv, pidx, hid, na, nm, rope, wqkv, wout, wgu, wdn, o,
           ring, k_b, v_b, dn_b, s_b,
           hid_v, na_v, nm_v, pidx_v, rope_v, x0, xf, xm, qbuf, psend, precv,
           abuf, mbuf, mrecv, maskx, mrow, snew, vnew_b,
           sm_sem, ring_sem, k_sem, v_sem, dn_sem,
           x0_s, x0_r, mk_s, mk_r, q_s, q_r, p_s, p_r, a_s, a_r, xm_s, xm_r, xf_s, xf_r, m_s, m_r):
    layers, pages, page_len, kv_heads, head_dim, rep_q, width, ffn, steps = dims
    per = HEADS_PER_GROUP
    groups = kv_heads // per
    tiles = page_len * per // 128
    slice_w = width // N_DEV
    q_w = rep_q * head_dim
    rows = rep_q * N_DEV
    scale2 = float(head_dim ** -0.5 * math.log2(math.e))

    me = lax.axis_index('pool')
    rep = lax.axis_index('replica')
    b0 = lax.rem(me, 2)
    b1 = lax.rem(me // 2, 2)
    b2 = me // 4

    def peer(k):
        return lax.rem(b0 + k % 2, 2) + 2 * lax.rem(b1 + (k // 2) % 2, 2) + 4 * lax.rem(b2 + k // 4, 2)

    def group_of(kx):
        return lax.rem(b2 + kx, 2)

    n_wq, n_wo = -(-(q_w + 2 * head_dim) // STEP), -(-slice_w // STEP)
    per_layer = n_wq + n_wo + 2 * steps

    def remote(src, dst, ssem, rsem, k):
        return pltpu.make_async_remote_copy(src_ref=src, dst_ref=dst, send_sem=ssem, recv_sem=rsem,
                                            device_id=(rep, peer(k)), device_id_type=MESH)

    FAR_FIRST = (6, 7, 4, 5, 2, 3, 1)

    def my_cols(ref, w):
        return ref.at[:, pl.ds(pl.multiple_of(me * w, 128), w)]

    def ring_slot(l, j):
        return lax.rem(l * per_layer + j, RING)

    def ring_copies(l, j):
        slot = ring_slot(l, j)

        def copy(i, src, off, w, at):
            return pltpu.make_async_copy(src.at[l, :, pl.ds(pl.multiple_of(off, 128), w)],
                                         ring.at[slot, :, pl.ds(at, w)], ring_sem.at[slot, i])

        if j < n_wq:
            lo, hi = j * STEP, (j + 1) * STEP
            parts, base = [], 0
            for off, w in ((me * q_w, q_w), (width + me * head_dim, head_dim),
                           (width + (kv_heads + me) * head_dim, head_dim)):
                x, y = max(lo, base), min(hi, base + w)
                if x < y:
                    parts.append((wqkv, off + x - base, y - x, x - lo))
                base += w
            return [copy(i, *p) for i, p in enumerate(parts)]
        if j < n_wq + n_wo:
            lo = (j - n_wq) * STEP
            return [copy(0, wout, me * slice_w + lo, min(STEP, slice_w - lo), 0)]
        s, part = divmod(j - n_wq - n_wo, 2)
        return [copy(0, wgu, part * ffn + ffn_base(me) + s * STEP, STEP, 0)]

    def refill(l, j):
        if j + RING < per_layer:
            start(ring_copies(l, j + RING))

    def kv_copies(l, which, buf, sem):
        return [pltpu.make_async_copy(kv.at[l, :, which, :, p], buf.at[p], sem.at[p]) for p in range(groups)]

    def ffn_base(dev):
        return 128 * ((dev * (ffn // 128)) // N_DEV)

    def dn_copies(l, s):
        return [pltpu.make_async_copy(
            wdn.at[l, pl.ds(pl.multiple_of(ffn_base(j) + s * STEP, 128), STEP),
                   pl.ds(pl.multiple_of(me * slice_w, 128), slice_w)],
            dn_b.at[s, pl.ds(j * STEP, STEP)], dn_sem.at[s, j]) for j in range(N_DEV)]

    def start(cps):
        for c in cps:
            c.start()

    def wait(cps):
        for c in cps:
            c.wait()

    small = [pltpu.make_async_copy(a, b, sm_sem.at[i]) for i, (a, b) in enumerate(
        ((hid, hid_v), (pidx.at[0], pidx_v), (na, na_v), (nm, nm_v), (rope, rope_v)))]
    start(small)
    for j in range(n_wq):
        start(ring_copies(0, j))

    barrier = pltpu.get_barrier_semaphore()
    for k in range(1, N_DEV):
        pl.semaphore_signal(barrier, inc=1, device_id=(rep, peer(k)), device_id_type=MESH)
    wait(small)
    x0[me] = hid_v[...].astype(F32)
    lane = lax.broadcasted_iota(jnp.int32, (N_DEV, 128), 1)
    idx = pidx_v[...]
    hit = lane < 0
    for j in range(idx.shape[1]):
        hit = jnp.logical_or(hit, idx[:, j:j + 1] == lane)
    hitf = jnp.where(hit, 1.0, 0.0).astype(F32)
    for owner in range(N_DEV):
        psend[owner, 0] = jnp.broadcast_to(hitf[owner:owner + 1, :], (N_DEV, 128))
    pl.semaphore_wait(barrier, N_DEV - 1)
    x0_cps = [remote(x0.at[me], x0.at[me], x0_s.at[k], x0_r.at[k], k) for k in FAR_FIRST]
    start(x0_cps)
    mk_cps = [remote(psend.at[peer(k), 0], mrecv.at[me], mk_s.at[k], mk_r.at[k], k) for k in FAR_FIRST]
    start(mk_cps)
    mrecv[me] = psend[me, 0]
    start(kv_copies(0, 0, k_b, k_sem))
    start(kv_copies(0, 1, v_b, v_sem))
    wait(x0_cps)
    sub8 = lax.broadcasted_iota(jnp.int32, (N_DEV, width), 0)
    xin = jnp.zeros((N_DEV, width), F32)
    for j in range(N_DEV):
        xin = jnp.where(sub8 == j, jnp.broadcast_to(x0[j], (N_DEV, width)), xin)
    xf[...] = xin.astype(BF16)

    head_lane = lax.rem(lax.broadcasted_iota(jnp.int32, (rows, 128), 1), per)
    grp = lax.broadcasted_iota(jnp.int32, (N_DEV, 128), 1) // 16
    low8 = lax.rem(lax.broadcasted_iota(jnp.int32, (N_DEV, 128), 1), 16) < 8

    def norm(x, gains, l):
        g = jnp.where(l == 0, gains[0:1, :].astype(F32), gains[1:2, :].astype(F32))
        inv = lax.rsqrt(jnp.sum(x * x, axis=-1, keepdims=True) / width + NORM_EPS)
        return (x * inv * g).astype(BF16)

    def layer(l, carry):
        h = norm(xf[...].astype(F32), na_v[...], l)
        us = []
        n_q = -(-q_w // STEP)
        for j in range(n_q):
            wait(ring_copies(l, j))
        for j in range(n_q):
            us.append(jnp.dot(h, ring[ring_slot(l, j)], preferred_element_type=F32))
        u = jnp.concatenate(us, axis=1).astype(BF16).astype(F32)
        cos = rope_v[0:1, :]
        sin = rope_v[1:2, :]

        def rot(v):
            return (v * cos + pltpu.roll(v, head_dim // 2, 1) * sin).astype(BF16)

        qs = [rot(u[:, g * head_dim:(g + 1) * head_dim]).astype(F32) for g in range(rep_q)]
        qbuf[me] = jnp.concatenate(qs, axis=0).astype(BF16)
        q_cps = {k: remote(qbuf.at[me], qbuf.at[me], q_s.at[k], q_r.at[k], k) for k in range(1, N_DEV)}
        start([q_cps[k] for k in FAR_FIRST])

        for j in range(n_q, n_wq):
            wait(ring_copies(l, j))
            w = min(STEP, q_w + 2 * head_dim - j * STEP)
            more = jnp.dot(h, ring[ring_slot(l, j), :, 0:w], preferred_element_type=F32)
            u = jnp.concatenate([u, more.astype(BF16).astype(F32)], axis=1)

        @pl.when(l == 0)
        def _():
            for j in range(n_wq, RING):
                start(ring_copies(0, j))

        for j in range(n_wq):
            refill(l, j)
        for s in range(steps):
            start(dn_copies(l, s))
        kn = rot(u[:, q_w:q_w + head_dim]).astype(F32)
        vnew_b[...] = u[:, q_w + head_dim:]
        for g in range(rep_q):
            snew[g] = jnp.broadcast_to(jnp.sum(qs[g] * kn, axis=-1, keepdims=True), (N_DEV, 128))

        @pl.when(l == 0)
        def _():
            wait(mk_cps)
            sub = lax.broadcasted_iota(jnp.int32, (N_DEV, 128), 0)
            mk = jnp.zeros((N_DEV, 128), F32)
            for r in range(N_DEV):
                mk = jnp.where(sub == r, mrecv[r], mk)
            for p in range(pages):
                maskx[p] = jnp.broadcast_to(mk[:, p:p + 1], (N_DEV, 128))

        wait(kv_copies(l, 0, k_b, k_sem))
        flat = SCORE_PAGES * page_len * per
        for kx in range(groups):
            for k in range(per * kx, per * (kx + 1)):
                if k:
                    q_cps[k].wait()
            p = group_of(kx)
            q_all = jnp.concatenate([qbuf[per * p + i] for i in range(per)], axis=0)

            def score_body(c, mx, p=p, q_all=q_all, kx=kx):
                kt = k_b[p, pl.ds(c * SCORE_PAGES, SCORE_PAGES)].reshape(flat, head_dim)
                s = lax.dot_general(q_all, kt, (((1,), (1,)), ((), ())), preferred_element_type=F32)
                for i in range(SCORE_PAGES):
                    keep = maskx[c * SCORE_PAGES + i] > 0.5
                    keep = jnp.concatenate([keep] * rep_q, axis=0)
                    for t in range(i * tiles, (i + 1) * tiles):
                        st = s[:, t * 128:(t + 1) * 128]
                        sp = st[(per - 1) * rows:]
                        for hh in range(per - 2, -1, -1):
                            sp = jnp.where(head_lane == hh, st[hh * rows:(hh + 1) * rows], sp)
                        sp = jnp.where(keep, sp, NEG)
                        s_b[kx, c * (SCORE_PAGES * tiles) + t] = sp
                        mx = jnp.maximum(mx, sp)
                return mx

            mx = lax.fori_loop(0, pages // SCORE_PAGES, score_body, jnp.full((rows, 128), NEG, F32))
            m = jnp.zeros((rows, 128), F32)
            for hh in range(per):
                m = jnp.where(head_lane == hh, jnp.max(jnp.where(head_lane == hh, mx, NEG), axis=-1, keepdims=True), m)
            mrow[kx] = m

        @pl.when(l + 1 < layers)
        def _():
            start(kv_copies(l + 1, 0, k_b, k_sem))

        wait(kv_copies(l, 1, v_b, v_sem))
        p_cps = {k: remote(psend.at[peer(k)], precv.at[me], p_s.at[k], p_r.at[k], k) for k in range(1, N_DEV)}
        for kx in reversed(range(groups)):
            p = group_of(kx)
            m = mrow[kx]

            def value_body(c, carry, p=p, m=m, kx=kx):
                acc, den = carry
                pieces = []
                for t in range(VALUE_PAGES * tiles):
                    e = jnp.exp2((s_b[kx, c * (VALUE_PAGES * tiles) + t] - m) * scale2)
                    den = den + e
                    pieces.append(jnp.concatenate([jnp.where(head_lane == hh, e, 0.0) for hh in range(per)], axis=0).astype(BF16))
                vt = v_b[p, pl.ds(c * VALUE_PAGES, VALUE_PAGES)].reshape(VALUE_PAGES * page_len * per, head_dim)
                acc = acc + jnp.dot(jnp.concatenate(pieces, axis=1), vt, preferred_element_type=F32)
                return acc, den

            acc, den = lax.fori_loop(0, pages // VALUE_PAGES, value_body,
                                     (jnp.zeros((per * rows, head_dim), F32), jnp.zeros((rows, 128), F32)))
            for hh in range(per):
                l_h = jnp.sum(jnp.where(head_lane == hh, den, 0.0), axis=-1, keepdims=True)
                m_h = jnp.max(jnp.where(head_lane == hh, m, NEG), axis=-1, keepdims=True)
                stat = jnp.zeros((N_DEV, 128), F32)
                for g in range(rep_q):
                    rs = slice(g * N_DEV, (g + 1) * N_DEV)
                    psend[per * p + hh, g] = acc[hh * rows + g * N_DEV:hh * rows + (g + 1) * N_DEV]
                    stat = jnp.where(grp == g, jnp.where(low8, m_h[rs], l_h[rs]), stat)
                psend[per * p + hh, rep_q] = stat
            for k in range(per * (kx + 1) - 1, per * kx - 1, -1):
                if k:
                    p_cps[k].start()
        precv[me] = psend[me]

        @pl.when(l + 1 < layers)
        def _():
            start(kv_copies(l + 1, 1, v_b, v_sem))

        wait([p_cps[k] for k in FAR_FIRST])
        stats = [precv[j, rep_q] for j in range(N_DEV)]
        heads_out = []
        for g in range(rep_q):
            ms = [jnp.broadcast_to(st[:, 16 * g:16 * g + 1], (N_DEV, 128)) for st in stats]
            ls = [jnp.broadcast_to(st[:, 16 * g + 8:16 * g + 9], (N_DEV, 128)) for st in stats]
            sn = snew[g]
            top = sn
            for mj in ms:
                top = jnp.maximum(top, mj)
            e_new = jnp.exp2((sn - top) * scale2)
            den = e_new
            num = jnp.zeros((N_DEV, head_dim), F32)
            for j in range(N_DEV):
                w = jnp.exp2((ms[j] - top) * scale2)
                den = den + w * ls[j]
                num = num + w * precv[j, g]
            p_new = (e_new / den).astype(BF16).astype(F32)
            heads_out.append(num / den + p_new * vnew_b[...])
        my_cols(abuf, q_w)[...] = jnp.concatenate(heads_out, axis=1).astype(BF16)
        a_cps = {k: remote(my_cols(abuf, q_w), my_cols(abuf, q_w), a_s.at[k], a_r.at[k], k) for k in range(1, N_DEV)}
        start([a_cps[k] for k in FAR_FIRST])

        for j in range(n_wo):
            wait(ring_copies(l, n_wq + j))
        projs = [None] * n_wo
        xm_cps = []

        def out_cols(j):
            return pl.ds(pl.multiple_of(me * slice_w + j * STEP, 128), min(STEP, slice_w - j * STEP))

        half = width // 2
        for kx in range(2):
            wait([a_cps[k] for k in range(4 * kx, 4 * kx + 4) if k])
            at = pl.ds(pl.multiple_of(group_of(kx) * half, 128), half)
            for j in range(n_wo):
                w = min(STEP, slice_w - j * STEP)
                d = jnp.dot(abuf[:, at], ring[ring_slot(l, n_wq + j), at, 0:w], preferred_element_type=F32)
                projs[j] = d if kx == 0 else projs[j] + d
                if kx:
                    cols = out_cols(j)
                    xm[:, cols] = (xf[:, cols].astype(F32) + projs[j]).astype(BF16)
                    cps = [remote(xm.at[:, cols], xm.at[:, cols], xm_s.at[j, k], xm_r.at[j, k], k) for k in FAR_FIRST]
                    start(cps)
                    xm_cps += cps
        for j in range(n_wo):
            refill(l, n_wq + j)
        wait(xm_cps)

        h2 = norm(xm[...].astype(F32), nm_v[...], l)
        mlane = lax.broadcasted_iota(jnp.int32, (N_DEV, STEP), 1)

        def m_cps(s):
            cols = pl.ds(pl.multiple_of(me * STEP, 128), STEP)
            return [remote(mbuf.at[s, :, cols], mbuf.at[s, :, cols], m_s.at[s, k], m_r.at[s, k], k) for k in FAR_FIRST]

        def activate(s, gate, up):
            gate = gate.astype(BF16).astype(F32)
            act = gate / (1.0 + jnp.exp(-gate)) * up.astype(BF16).astype(F32)
            if s == 0:
                act = jnp.where(jnp.logical_and(b0 == 1, mlane < 128), 0.0, act)
            mbuf[s, :, pl.ds(pl.multiple_of(me * STEP, 128), STEP)] = act.astype(BF16)

        before = None
        for s in range(steps):
            j = n_wq + n_wo + 2 * s
            wait(ring_copies(l, j))
            wait(ring_copies(l, j + 1))
            gate = jnp.dot(h2, ring[ring_slot(l, j)], preferred_element_type=F32)
            up = jnp.dot(h2, ring[ring_slot(l, j + 1)], preferred_element_type=F32)
            if s:
                activate(s - 1, *before)
                start(m_cps(s - 1))
            before = (gate, up)
            refill(l, j)
            refill(l, j + 1)
        activate(steps - 1, *before)
        start(m_cps(steps - 1))

        @pl.when(l + 1 < layers)
        def _():
            for j in range(n_wq):
                start(ring_copies(l + 1, j))

        def down_step(s):
            wait(dn_copies(l, s))
            wait(m_cps(s))

        def down_body(i, acc):
            down_step(2 * i)
            down_step(2 * i + 1)
            acc = (acc + jnp.dot(mbuf[2 * i], dn_b[2 * i], preferred_element_type=F32)
                   + jnp.dot(mbuf[2 * i + 1], dn_b[2 * i + 1], preferred_element_type=F32))
            return acc

        acc = lax.fori_loop(0, steps // 2, down_body, jnp.zeros((N_DEV, slice_w), F32))
        tail = steps - steps % 2
        for st in range(tail, steps):
            down_step(st)
        xf_cps, news = [], []
        for j in range(n_wo):
            lo, hi = j * STEP, min((j + 1) * STEP, slice_w)
            part = acc[:, lo:hi]
            for st in range(tail, steps):
                part = part + jnp.dot(mbuf[st], dn_b[st, :, lo:hi], preferred_element_type=F32)
            cols = out_cols(j)
            new = (xm[:, cols].astype(F32) + part).astype(BF16)
            news.append(new)
            cps = [remote(xf.at[:, cols], xf.at[:, cols], xf_s.at[j, k], xf_r.at[j, k], k) for k in FAR_FIRST]
            xf_cps += cps

            @pl.when(l + 1 < layers)
            def _(new=new, cols=cols, cps=cps):
                xf[:, cols] = new
                start(cps)

        @pl.when(l + 1 < layers)
        def _():
            for j in range(n_wq, RING):
                start(ring_copies(l + 1, j))
            wait(xf_cps)

        @pl.when(l + 1 == layers)
        def _():
            row = jnp.concatenate(news, axis=1).astype(F32)
            for r in range(N_DEV):
                x0[r, :, slice_w:2 * slice_w] = row[r:r + 1]
            cps = [remote(x0.at[peer(k), :, pl.ds(slice_w, slice_w)], x0.at[me, :, pl.ds(0, slice_w)],
                          x0_s.at[k], x0_r.at[k], k) for k in FAR_FIRST]
            start(cps)
            x0[me, :, 0:slice_w] = x0[me, :, slice_w:2 * slice_w]
            wait(cps)
            for j in range(N_DEV):
                o[:, j * slice_w:(j + 1) * slice_w] = x0[j, :, 0:slice_w].astype(BF16)
        return carry

    lax.fori_loop(0, layers, layer, 0)


def solution(mesh):
    def device_fn(kv_pool, page_idx, hidden, norm_attn, norm_mlp, w_qkv, w_out, w_gate_up, w_down):
        layers, pages, _, page_len, kv_heads, head_dim = kv_pool.shape
        group, take = page_idx.shape[1:]
        width = hidden.shape[1]
        ffn = w_down.shape[1]
        rep_q = (w_qkv.shape[2] - 2 * kv_heads * head_dim) // head_dim // kv_heads
        rows = rep_q * group
        slice_w = width // group
        q_w = rep_q * head_dim
        steps = -(-(-(-(ffn // 128) // group)) // (STEP // 128))
        position = float(group * take * page_len)
        n_out = -(-slice_w // STEP)
        rope = jnp.asarray(rope_table(position, head_dim))
        groups = kv_heads // HEADS_PER_GROUP
        kv = kv_pool.reshape(layers, pages, 2, page_len, groups, HEADS_PER_GROUP, head_dim)
        dims = (layers, pages, page_len, kv_heads, head_dim, rep_q, width, ffn, steps)
        dma = pltpu.SemaphoreType.DMA
        any_spec = pl.BlockSpec(memory_space=pl.ANY)
        tiles = page_len * HEADS_PER_GROUP // 128
        return pl.pallas_call(
            functools.partial(kernel, dims),
            out_shape=jax.ShapeDtypeStruct((1, width), BF16),
            in_specs=[any_spec] * 10,
            out_specs=pl.BlockSpec(memory_space=pltpu.VMEM),
            scratch_shapes=[
                pltpu.VMEM((RING, width, STEP), BF16),
                pltpu.VMEM((groups, pages, page_len, HEADS_PER_GROUP, head_dim), BF16),
                pltpu.VMEM((groups, pages, page_len, HEADS_PER_GROUP, head_dim), BF16),
                pltpu.VMEM((steps, group * STEP, slice_w), BF16),
                pltpu.VMEM((groups, pages * tiles, rows, 128), F32),
                pltpu.VMEM((1, width), BF16),
                pltpu.VMEM((layers, width), BF16),
                pltpu.VMEM((layers, width), BF16),
                pltpu.VMEM((group, take), jnp.int32),
                pltpu.VMEM((2, head_dim), F32),
                pltpu.VMEM((group, 1, width), F32),
                pltpu.VMEM((group, width), BF16),
                pltpu.VMEM((group, width), BF16),
                pltpu.VMEM((group, rows, head_dim), BF16),
                pltpu.VMEM((group, rep_q + 1, group, 128), F32),
                pltpu.VMEM((group, rep_q + 1, group, 128), F32),
                pltpu.VMEM((group, width), BF16),
                pltpu.VMEM((steps, group, group * STEP), BF16),
                pltpu.VMEM((group, group, 128), F32),
                pltpu.VMEM((pages, group, 128), F32),
                pltpu.VMEM((groups, rows, 128), F32),
                pltpu.VMEM((rep_q, group, 128), F32),
                pltpu.VMEM((group, head_dim), F32),
                dma((5,)), dma((RING, 2)), dma((groups,)), dma((groups,)), dma((steps, group)),
            ] + [dma((group,))] * 10 + [dma((n_out, group))] * 4 + [dma((steps, group))] * 2,
            compiler_params=pltpu.CompilerParams(
                collective_id=0, has_side_effects=True, vmem_limit_bytes=67_043_328),
            name="decode_step",
        )(kv, page_idx, hidden, norm_attn, norm_mlp, rope, w_qkv, w_out, w_gate_up, w_down)

    row_spec = P(('replica', 'pool'))
    in_specs = (P(None, ('replica', 'pool')), row_spec, row_spec, P(), P(), P(), P(), P(), P())
    return jax.shard_map(device_fn, mesh=mesh, in_specs=in_specs, out_specs=row_spec, check_vma=False)
```

```python
import functools
import math

import jax
import jax.numpy as jnp
import numpy as np
from jax import lax
from jax.experimental import pallas as pl
from jax.experimental.pallas import tpu as pltpu
from jax.sharding import PartitionSpec as P

NORM_EPS = 1e-5
ROPE_BASE = 500000.0
NEG = -3.0e38
MESH = pl.DeviceIdType.MESH
F32 = jnp.float32
BF16 = jnp.bfloat16

N_DEV = 8
RING = 8
STEP = 256
HEADS_PER_GROUP = 4
SCORE_PAGES = 32
VALUE_PAGES = 32
DOT_PAGES = 8


def rope_table(position, head_dim):
    half = head_dim // 2
    freq = ROPE_BASE ** (-np.arange(half, dtype=np.float64) * 2.0 / head_dim)
    angle = position * freq
    cos = np.concatenate([np.cos(angle), np.cos(angle)])
    sin = np.concatenate([-np.sin(angle), np.sin(angle)])
    return np.stack([cos, sin]).astype(np.float32)


def kernel(dims, kv, pidx, hid, na, nm, rope, wqkv, wout, wgu, wdn, o,
           ring, k_b, v_b, dn_b, s_b,
           hid_v, na_v, nm_v, pidx_v, rope_v, x0, xf, xm, qbuf, psend, precv,
           abuf, mbuf, mrecv, maskx, mrow, snew, vnew_b,
           sm_sem, ring_sem, k_sem, v_sem, dn_sem,
           x0_s, x0_r, mk_s, mk_r, q_s, q_r, p_s, p_r, a_s, a_r, xm_s, xm_r, xf_s, xf_r, m_s, m_r):
    layers, pages, page_len, kv_heads, head_dim, rep_q, width, ffn, steps = dims
    per = HEADS_PER_GROUP
    groups = kv_heads // per
    tiles = page_len * per // 128
    slice_w = width // N_DEV
    q_w = rep_q * head_dim
    rows = rep_q * N_DEV
    scale2 = float(head_dim ** -0.5 * math.log2(math.e))

    me = lax.axis_index('pool')
    rep = lax.axis_index('replica')
    b0 = lax.rem(me, 2)
    b1 = lax.rem(me // 2, 2)
    b2 = me // 4

    def peer(k):
        return lax.rem(b0 + k % 2, 2) + 2 * lax.rem(b1 + (k // 2) % 2, 2) + 4 * lax.rem(b2 + k // 4, 2)

    def group_of(kx):
        return lax.rem(b2 + kx, 2)

    n_wq, n_wo = -(-(q_w + 2 * head_dim) // STEP), -(-slice_w // STEP)
    per_layer = n_wq + n_wo + 2 * steps

    def remote(src, dst, ssem, rsem, k):
        return pltpu.make_async_remote_copy(src_ref=src, dst_ref=dst, send_sem=ssem, recv_sem=rsem,
                                            device_id=(rep, peer(k)), device_id_type=MESH)

    FAR_FIRST = (6, 7, 4, 5, 2, 3, 1)

    def my_cols(ref, w):
        return ref.at[:, pl.ds(pl.multiple_of(me * w, 128), w)]

    def ring_slot(l, j):
        return lax.rem(l * per_layer + j, RING)

    def ring_copies(l, j):
        slot = ring_slot(l, j)

        def copy(i, src, off, w, at):
            return pltpu.make_async_copy(src.at[l, :, pl.ds(pl.multiple_of(off, 128), w)],
                                         ring.at[slot, :, pl.ds(at, w)], ring_sem.at[slot, i])

        if j < n_wq:
            lo, hi = j * STEP, (j + 1) * STEP
            parts, base = [], 0
            for off, w in ((me * q_w, q_w), (width + me * head_dim, head_dim),
                           (width + (kv_heads + me) * head_dim, head_dim)):
                x, y = max(lo, base), min(hi, base + w)
                if x < y:
                    parts.append((wqkv, off + x - base, y - x, x - lo))
                base += w
            return [copy(i, *p) for i, p in enumerate(parts)]
        if j < n_wq + n_wo:
            lo = (j - n_wq) * STEP
            return [copy(0, wout, me * slice_w + lo, min(STEP, slice_w - lo), 0)]
        s, part = divmod(j - n_wq - n_wo, 2)
        return [copy(0, wgu, part * ffn + ffn_base(me) + s * STEP, STEP, 0)]

    def refill(l, j):
        if j + RING < per_layer:
            start(ring_copies(l, j + RING))

    def kv_copies(l, which, buf, sem):
        return [pltpu.make_async_copy(kv.at[l, :, which, :, p], buf.at[p], sem.at[p]) for p in range(groups)]

    def ffn_base(dev):
        return 128 * ((dev * (ffn // 128)) // N_DEV)

    def dn_copies(l, s):
        return [pltpu.make_async_copy(
            wdn.at[l, pl.ds(pl.multiple_of(ffn_base(j) + s * STEP, 128), STEP),
                   pl.ds(pl.multiple_of(me * slice_w, 128), slice_w)],
            dn_b.at[s, pl.ds(j * STEP, STEP)], dn_sem.at[s, j]) for j in range(N_DEV)]

    def start(cps):
        for c in cps:
            c.start()

    def wait(cps):
        for c in cps:
            c.wait()

    small = [pltpu.make_async_copy(a, b, sm_sem.at[i]) for i, (a, b) in enumerate(
        ((hid, hid_v), (pidx.at[0], pidx_v), (na, na_v), (nm, nm_v), (rope, rope_v)))]
    start(small)
    for j in range(n_wq):
        start(ring_copies(0, j))

    barrier = pltpu.get_barrier_semaphore()
    for k in range(1, N_DEV):
        pl.semaphore_signal(barrier, inc=1, device_id=(rep, peer(k)), device_id_type=MESH)
    wait(small)
    x0[me] = hid_v[...].astype(F32)
    lane = lax.broadcasted_iota(jnp.int32, (N_DEV, 128), 1)
    idx = pidx_v[...]
    hit = lane < 0
    for j in range(idx.shape[1]):
        hit = jnp.logical_or(hit, idx[:, j:j + 1] == lane)
    hitf = jnp.where(hit, 1.0, 0.0).astype(F32)
    for owner in range(N_DEV):
        psend[owner, 0] = jnp.broadcast_to(hitf[owner:owner + 1, :], (N_DEV, 128))
    pl.semaphore_wait(barrier, N_DEV - 1)
    x0_cps = [remote(x0.at[me], x0.at[me], x0_s.at[k], x0_r.at[k], k) for k in FAR_FIRST]
    start(x0_cps)
    mk_cps = [remote(psend.at[peer(k), 0], mrecv.at[me], mk_s.at[k], mk_r.at[k], k) for k in FAR_FIRST]
    start(mk_cps)
    mrecv[me] = psend[me, 0]
    start(kv_copies(0, 0, k_b, k_sem))
    start(kv_copies(0, 1, v_b, v_sem))
    wait(x0_cps)
    sub8 = lax.broadcasted_iota(jnp.int32, (N_DEV, width), 0)
    xin = jnp.zeros((N_DEV, width), F32)
    for j in range(N_DEV):
        xin = jnp.where(sub8 == j, jnp.broadcast_to(x0[j], (N_DEV, width)), xin)
    xf[...] = xin.astype(BF16)

    head_lane = lax.rem(lax.broadcasted_iota(jnp.int32, (rows, 128), 1), per)
    grp = lax.broadcasted_iota(jnp.int32, (N_DEV, 128), 1) // 16
    low8 = lax.rem(lax.broadcasted_iota(jnp.int32, (N_DEV, 128), 1), 16) < 8

    def norm(x, gains, l):
        g = jnp.where(l == 0, gains[0:1, :].astype(F32), gains[1:2, :].astype(F32))
        inv = lax.rsqrt(jnp.sum(x * x, axis=-1, keepdims=True) / width + NORM_EPS)
        return (x * inv * g).astype(BF16)

    def layer(l, carry):
        h = norm(xf[...].astype(F32), na_v[...], l)
        us = []
        n_q = -(-q_w // STEP)
        for j in range(n_q):
            wait(ring_copies(l, j))
        for j in range(n_q):
            us.append(jnp.dot(h, ring[ring_slot(l, j)], preferred_element_type=F32))
        u = jnp.concatenate(us, axis=1).astype(BF16).astype(F32)
        cos = rope_v[0:1, :]
        sin = rope_v[1:2, :]

        def rot(v):
            return (v * cos + pltpu.roll(v, head_dim // 2, 1) * sin).astype(BF16)

        qs = [rot(u[:, g * head_dim:(g + 1) * head_dim]).astype(F32) for g in range(rep_q)]
        qbuf[me] = jnp.concatenate(qs, axis=0).astype(BF16)
        q_cps = {k: remote(qbuf.at[me], qbuf.at[me], q_s.at[k], q_r.at[k], k) for k in range(1, N_DEV)}
        start([q_cps[k] for k in FAR_FIRST])

        for j in range(n_q, n_wq):
            wait(ring_copies(l, j))
            w = min(STEP, q_w + 2 * head_dim - j * STEP)
            more = jnp.dot(h, ring[ring_slot(l, j), :, 0:w], preferred_element_type=F32)
            u = jnp.concatenate([u, more.astype(BF16).astype(F32)], axis=1)

        @pl.when(l == 0)
        def _():
            for j in range(n_wq, RING):
                start(ring_copies(0, j))

        for j in range(n_wq):
            refill(l, j)
        for s in range(steps):
            start(dn_copies(l, s))
        kn = rot(u[:, q_w:q_w + head_dim]).astype(F32)
        vnew_b[...] = u[:, q_w + head_dim:]
        for g in range(rep_q):
            snew[g] = jnp.broadcast_to(jnp.sum(qs[g] * kn, axis=-1, keepdims=True), (N_DEV, 128))

        @pl.when(l == 0)
        def _():
            wait(mk_cps)
            sub = lax.broadcasted_iota(jnp.int32, (N_DEV, 128), 0)
            mk = jnp.zeros((N_DEV, 128), F32)
            for r in range(N_DEV):
                mk = jnp.where(sub == r, mrecv[r], mk)
            for p in range(pages):
                maskx[p] = jnp.broadcast_to(mk[:, p:p + 1], (N_DEV, 128)).astype(BF16)

        wait(kv_copies(l, 0, k_b, k_sem))
        flat = DOT_PAGES * page_len * per
        for kx in range(groups):
            for k in range(per * kx, per * (kx + 1)):
                if k:
                    q_cps[k].wait()
            p = group_of(kx)
            q_all = jnp.concatenate([qbuf[per * p + i] for i in range(per)], axis=0)

            def score_body(c, mx, p=p, q_all=q_all, kx=kx):
                for i in range(SCORE_PAGES):
                    if i % DOT_PAGES == 0:
                        kt = k_b[p, pl.ds(c * SCORE_PAGES + i, DOT_PAGES)].reshape(flat, head_dim)
                        s = lax.dot_general(q_all, kt, (((1,), (1,)), ((), ())), preferred_element_type=F32)
                    keep = maskx[c * SCORE_PAGES + i].astype(F32) > 0.5
                    keep = jnp.concatenate([keep] * rep_q, axis=0)
                    for t in range(i * tiles, (i + 1) * tiles):
                        lo = (t % (DOT_PAGES * tiles)) * 128
                        st = s[:, lo:lo + 128]
                        sp = st[(per - 1) * rows:]
                        for hh in range(per - 2, -1, -1):
                            sp = jnp.where(head_lane == hh, st[hh * rows:(hh + 1) * rows], sp)
                        sp = jnp.where(keep, sp, NEG)
                        s_b[kx, c * (SCORE_PAGES * tiles) + t] = sp
                        mx = jnp.maximum(mx, sp)
                return mx

            mx = lax.fori_loop(0, pages // SCORE_PAGES, score_body, jnp.full((rows, 128), NEG, F32))
            m = jnp.zeros((rows, 128), F32)
            for hh in range(per):
                m = jnp.where(head_lane == hh, jnp.max(jnp.where(head_lane == hh, mx, NEG), axis=-1, keepdims=True), m)
            mrow[kx] = m

        @pl.when(l + 1 < layers)
        def _():
            start(kv_copies(l + 1, 0, k_b, k_sem))

        wait(kv_copies(l, 1, v_b, v_sem))
        p_cps = {k: remote(psend.at[peer(k)], precv.at[me], p_s.at[k], p_r.at[k], k) for k in range(1, N_DEV)}
        for kx in reversed(range(groups)):
            p = group_of(kx)
            m = mrow[kx]

            def value_body(c, carry, p=p, m=m, kx=kx):
                acc, den = carry
                for d in range(0, VALUE_PAGES, DOT_PAGES):
                    pieces = []
                    for t in range(d * tiles, (d + DOT_PAGES) * tiles):
                        e = jnp.exp2((s_b[kx, c * (VALUE_PAGES * tiles) + t] - m) * scale2)
                        den = den + e
                        pieces.append(jnp.concatenate([jnp.where(head_lane == hh, e, 0.0) for hh in range(per)], axis=0).astype(BF16))
                    vt = v_b[p, pl.ds(c * VALUE_PAGES + d, DOT_PAGES)].reshape(flat, head_dim)
                    acc = acc + jnp.dot(jnp.concatenate(pieces, axis=1), vt, preferred_element_type=F32)
                return acc, den

            acc, den = lax.fori_loop(0, pages // VALUE_PAGES, value_body,
                                     (jnp.zeros((per * rows, head_dim), F32), jnp.zeros((rows, 128), F32)))
            for hh in range(per):
                l_h = jnp.sum(jnp.where(head_lane == hh, den, 0.0), axis=-1, keepdims=True)
                m_h = jnp.max(jnp.where(head_lane == hh, m, NEG), axis=-1, keepdims=True)
                stat = jnp.zeros((N_DEV, 128), F32)
                for g in range(rep_q):
                    rs = slice(g * N_DEV, (g + 1) * N_DEV)
                    psend[per * p + hh, g] = acc[hh * rows + g * N_DEV:hh * rows + (g + 1) * N_DEV]
                    stat = jnp.where(grp == g, jnp.where(low8, m_h[rs], l_h[rs]), stat)
                psend[per * p + hh, rep_q] = stat
            for k in range(per * (kx + 1) - 1, per * kx - 1, -1):
                if k:
                    p_cps[k].start()
        precv[me] = psend[me]

        @pl.when(l + 1 < layers)
        def _():
            start(kv_copies(l + 1, 1, v_b, v_sem))

        wait([p_cps[k] for k in FAR_FIRST])
        stats = [precv[j, rep_q] for j in range(N_DEV)]
        heads_out = []
        for g in range(rep_q):
            ms = [jnp.broadcast_to(st[:, 16 * g:16 * g + 1], (N_DEV, 128)) for st in stats]
            ls = [jnp.broadcast_to(st[:, 16 * g + 8:16 * g + 9], (N_DEV, 128)) for st in stats]
            sn = snew[g]
            top = sn
            for mj in ms:
                top = jnp.maximum(top, mj)
            e_new = jnp.exp2((sn - top) * scale2)
            den = e_new
            num = jnp.zeros((N_DEV, head_dim), F32)
            for j in range(N_DEV):
                w = jnp.exp2((ms[j] - top) * scale2)
                den = den + w * ls[j]
                num = num + w * precv[j, g]
            p_new = (e_new / den).astype(BF16).astype(F32)
            heads_out.append(num / den + p_new * vnew_b[...])
        my_cols(abuf, q_w)[...] = jnp.concatenate(heads_out, axis=1).astype(BF16)
        a_cps = {k: remote(my_cols(abuf, q_w), my_cols(abuf, q_w), a_s.at[k], a_r.at[k], k) for k in range(1, N_DEV)}
        start([a_cps[k] for k in FAR_FIRST])

        for j in range(n_wo):
            wait(ring_copies(l, n_wq + j))
        projs = [None] * n_wo
        xm_cps = []

        def out_cols(j):
            return pl.ds(pl.multiple_of(me * slice_w + j * STEP, 128), min(STEP, slice_w - j * STEP))

        half = width // 2
        for kx in range(2):
            wait([a_cps[k] for k in range(4 * kx, 4 * kx + 4) if k])
            at = pl.ds(pl.multiple_of(group_of(kx) * half, 128), half)
            for j in range(n_wo):
                w = min(STEP, slice_w - j * STEP)
                d = jnp.dot(abuf[:, at], ring[ring_slot(l, n_wq + j), at, 0:w], preferred_element_type=F32)
                projs[j] = d if kx == 0 else projs[j] + d
                if kx:
                    cols = out_cols(j)
                    xm[:, cols] = (xf[:, cols].astype(F32) + projs[j]).astype(BF16)
                    cps = [remote(xm.at[:, cols], xm.at[:, cols], xm_s.at[j, k], xm_r.at[j, k], k) for k in FAR_FIRST]
                    start(cps)
                    xm_cps += cps
        for j in range(n_wo):
            refill(l, n_wq + j)
        wait(xm_cps)

        h2 = norm(xm[...].astype(F32), nm_v[...], l)
        mlane = lax.broadcasted_iota(jnp.int32, (N_DEV, STEP), 1)

        def m_cps(s):
            cols = pl.ds(pl.multiple_of(me * STEP, 128), STEP)
            return [remote(mbuf.at[s, :, cols], mbuf.at[s, :, cols], m_s.at[s, k], m_r.at[s, k], k) for k in FAR_FIRST]

        def activate(s, gate, up):
            gate = gate.astype(BF16).astype(F32)
            act = gate / (1.0 + jnp.exp(-gate)) * up.astype(BF16).astype(F32)
            if s == 0:
                act = jnp.where(jnp.logical_and(b0 == 1, mlane < 128), 0.0, act)
            mbuf[s, :, pl.ds(pl.multiple_of(me * STEP, 128), STEP)] = act.astype(BF16)

        before = None
        for s in range(steps):
            j = n_wq + n_wo + 2 * s
            wait(ring_copies(l, j))
            wait(ring_copies(l, j + 1))
            gate = jnp.dot(h2, ring[ring_slot(l, j)], preferred_element_type=F32)
            up = jnp.dot(h2, ring[ring_slot(l, j + 1)], preferred_element_type=F32)
            if s:
                activate(s - 1, *before)
                start(m_cps(s - 1))
            before = (gate, up)
            refill(l, j)
            refill(l, j + 1)
        activate(steps - 1, *before)
        start(m_cps(steps - 1))

        @pl.when(l + 1 < layers)
        def _():
            for j in range(n_wq):
                start(ring_copies(l + 1, j))

        def down_step(s):
            wait(dn_copies(l, s))
            wait(m_cps(s))

        def down_body(i, acc):
            down_step(2 * i)
            down_step(2 * i + 1)
            acc = (acc + jnp.dot(mbuf[2 * i], dn_b[2 * i], preferred_element_type=F32)
                   + jnp.dot(mbuf[2 * i + 1], dn_b[2 * i + 1], preferred_element_type=F32))
            return acc

        acc = lax.fori_loop(0, steps // 2, down_body, jnp.zeros((N_DEV, slice_w), F32))
        tail = steps - steps % 2
        for st in range(tail, steps):
            down_step(st)
        xf_cps, news = [], []
        for j in range(n_wo):
            lo, hi = j * STEP, min((j + 1) * STEP, slice_w)
            part = acc[:, lo:hi]
            for st in range(tail, steps):
                part = part + jnp.dot(mbuf[st], dn_b[st, :, lo:hi], preferred_element_type=F32)
            cols = out_cols(j)
            new = (xm[:, cols].astype(F32) + part).astype(BF16)
            news.append(new)
            cps = [remote(xf.at[:, cols], xf.at[:, cols], xf_s.at[j, k], xf_r.at[j, k], k) for k in FAR_FIRST]
            xf_cps += cps

            @pl.when(l + 1 < layers)
            def _(new=new, cols=cols, cps=cps):
                xf[:, cols] = new
                start(cps)

        @pl.when(l + 1 < layers)
        def _():
            for j in range(n_wq, RING):
                start(ring_copies(l + 1, j))
            wait(xf_cps)

        @pl.when(l + 1 == layers)
        def _():
            row = jnp.concatenate(news, axis=1).astype(F32)
            for r in range(N_DEV):
                x0[r, :, slice_w:2 * slice_w] = row[r:r + 1]
            cps = [remote(x0.at[peer(k), :, pl.ds(slice_w, slice_w)], x0.at[me, :, pl.ds(0, slice_w)],
                          x0_s.at[k], x0_r.at[k], k) for k in FAR_FIRST]
            start(cps)
            x0[me, :, 0:slice_w] = x0[me, :, slice_w:2 * slice_w]
            wait(cps)
            for j in range(N_DEV):
                o[:, j * slice_w:(j + 1) * slice_w] = x0[j, :, 0:slice_w].astype(BF16)
        return carry

    lax.fori_loop(0, layers, layer, 0)


def solution(mesh):
    def device_fn(kv_pool, page_idx, hidden, norm_attn, norm_mlp, w_qkv, w_out, w_gate_up, w_down):
        layers, pages, _, page_len, kv_heads, head_dim = kv_pool.shape
        group, take = page_idx.shape[1:]
        width = hidden.shape[1]
        ffn = w_down.shape[1]
        rep_q = (w_qkv.shape[2] - 2 * kv_heads * head_dim) // head_dim // kv_heads
        rows = rep_q * group
        slice_w = width // group
        q_w = rep_q * head_dim
        steps = -(-(-(-(ffn // 128) // group)) // (STEP // 128))
        position = float(group * take * page_len)
        n_out = -(-slice_w // STEP)
        rope = jnp.asarray(rope_table(position, head_dim))
        groups = kv_heads // HEADS_PER_GROUP
        kv = kv_pool.reshape(layers, pages, 2, page_len, groups, HEADS_PER_GROUP, head_dim)
        dims = (layers, pages, page_len, kv_heads, head_dim, rep_q, width, ffn, steps)
        dma = pltpu.SemaphoreType.DMA
        any_spec = pl.BlockSpec(memory_space=pl.ANY)
        tiles = page_len * HEADS_PER_GROUP // 128
        return pl.pallas_call(
            functools.partial(kernel, dims),
            out_shape=jax.ShapeDtypeStruct((1, width), BF16),
            in_specs=[any_spec] * 10,
            out_specs=pl.BlockSpec(memory_space=pltpu.VMEM),
            scratch_shapes=[
                pltpu.VMEM((RING, width, STEP), BF16),
                pltpu.VMEM((groups, pages, page_len, HEADS_PER_GROUP, head_dim), BF16),
                pltpu.VMEM((groups, pages, page_len, HEADS_PER_GROUP, head_dim), BF16),
                pltpu.VMEM((steps, group * STEP, slice_w), BF16),
                pltpu.VMEM((groups, pages * tiles, rows, 128), F32),
                pltpu.VMEM((1, width), BF16),
                pltpu.VMEM((layers, width), BF16),
                pltpu.VMEM((layers, width), BF16),
                pltpu.VMEM((group, take), jnp.int32),
                pltpu.VMEM((2, head_dim), F32),
                pltpu.VMEM((group, 1, width), F32),
                pltpu.VMEM((group, width), BF16),
                pltpu.VMEM((group, width), BF16),
                pltpu.VMEM((group, rows, head_dim), BF16),
                pltpu.VMEM((group, rep_q + 1, group, 128), F32),
                pltpu.VMEM((group, rep_q + 1, group, 128), F32),
                pltpu.VMEM((group, width), BF16),
                pltpu.VMEM((steps, group, group * STEP), BF16),
                pltpu.VMEM((group, group, 128), F32),
                pltpu.VMEM((pages, group, 128), BF16),
                pltpu.VMEM((groups, rows, 128), F32),
                pltpu.VMEM((rep_q, group, 128), F32),
                pltpu.VMEM((group, head_dim), F32),
                dma((5,)), dma((RING, 2)), dma((groups,)), dma((groups,)), dma((steps, group)),
            ] + [dma((group,))] * 10 + [dma((n_out, group))] * 4 + [dma((steps, group))] * 2,
            compiler_params=pltpu.CompilerParams(
                collective_id=0, has_side_effects=True, vmem_limit_bytes=67_043_328),
            name="decode_step",
        )(kv, page_idx, hidden, norm_attn, norm_mlp, rope, w_qkv, w_out, w_gate_up, w_down)

    row_spec = P(('replica', 'pool'))
    in_specs = (P(None, ('replica', 'pool')), row_spec, row_spec, P(), P(), P(), P(), P(), P())
    return jax.shard_map(device_fn, mesh=mesh, in_specs=in_specs, out_specs=row_spec, check_vma=False)
```
